16 devices in a mesh: dp: 1, sp: 16 (over x, y, z, core).
Axes of the slice: x: 2, y: 2, z: 2, core: 2. Of those that a mesh axis runs over, the one named last changes fastest.
Arguments:
- q: bfloat16 [32, 16, 128], P('dp')
- k: bfloat16 [32, 8192, 16, 128], P('dp', 'sp')
- v: bfloat16 [32, 8192, 16, 128], P('dp', 'sp')
Outputs:
- q: bfloat16 [32, 16, 128], P('dp')
All inputs are finite; a program needn't handle non-finite values.
Results may differ from the reference program's by a relative error of at most 0.012.
Values are sent between devices in bfloat16 or wider.
A program may use at most 2 GiB of HBM per device.

```python
import jax
import jax.numpy as jnp

BATCH = 32
CACHE = 8192
HEADS = 16
KV_HEADS = 16
HEAD = 128


def setup_inputs(seed: int = 0, part: int = 0) -> dict:
    kq, kk, kv = (jax.random.fold_in(k, part) for k in jax.random.split(jax.random.key(seed), 3))
    return {
        "q": (3 * jax.random.normal(kq, (BATCH, HEADS, HEAD), jnp.float32)).astype(jnp.bfloat16),
        "k": jax.random.normal(kk, (BATCH, CACHE, KV_HEADS, HEAD), jnp.float32).astype(jnp.bfloat16),
        "v": jax.random.normal(kv, (BATCH, CACHE, KV_HEADS, HEAD), jnp.float32).astype(jnp.bfloat16),
    }


def einsum(form, a, b):
    return jnp.einsum(form, a.astype(jnp.float32), b.astype(jnp.float32))


def reference(q, k, v):
    grouped = q.reshape(BATCH, KV_HEADS, -1, HEAD)
    scores = einsum("bgsd,bugd->bgsu", grouped, k) * HEAD**-0.5
    weights = jax.nn.softmax(scores, -1).astype(jnp.bfloat16)
    return einsum("bgsu,bugd->bgsd", weights, v).astype(jnp.bfloat16).reshape(BATCH, HEADS, HEAD)
```

```python
import functools, math
import jax, jax.numpy as jnp
from jax import lax
from jax.experimental import pallas as pl
from jax.experimental.pallas import tpu as pltpu
from jax.sharding import PartitionSpec as P

LOG2E = math.log2(math.e)
SLOTS = 4
MODE = "full"
SCALE = 128 ** -0.5 * LOG2E

def scores(w_ref, k):
    k4 = k.reshape(32, 8, 16, 128)
    lhs = jnp.concatenate([k4[:, t].reshape(512, 128) for t in range(8)], -1)
    s = lax.dot_general(lhs, w_ref[...], (((1,), (1,)), ((), ())), preferred_element_type=jnp.float32)
    return s.reshape(32, 16, 128)

def weigh(s, scale):
    row = lax.broadcasted_iota(jnp.int32, (16, 128), 0)
    col = lax.broadcasted_iota(jnp.int32, (16, 128), 1)
    mask = lax.rem(col, 16) == row
    top = jnp.max(s, 0)
    high = jnp.max(jnp.where(mask, top, -jnp.inf), -1, keepdims=True)
    p = jnp.where(mask[None], jnp.exp2(s * scale - high * scale), 0.0)
    total = jnp.sum(jnp.sum(p, 0), -1, keepdims=True)
    return p.astype(jnp.bfloat16), high, total

def mix(p, v):
    v2 = v.reshape(2, 2048, 128)
    rhs = jnp.concatenate([v2[0], v2[1]], -1)
    a = jnp.concatenate([p[g] for g in range(16)], -1)
    b = jnp.concatenate([p[g] for g in range(16, 32)], -1)
    lhs = jnp.concatenate([a, b], 0)
    r = jnp.dot(lhs, rhs, preferred_element_type=jnp.float32)
    return r[:16, :128] + r[16:, 128:]

MESH = pl.DeviceIdType.MESH
GROUP = 4


def combine(racc, rst, o_ref, b):
    rows = rst[:, b]
    top = jnp.max(rows, 0, keepdims=True)
    scale = jnp.exp2((rows - top) * SCALE)
    sums = pltpu.roll(rows, 112, 2)
    w = scale / jnp.sum(scale * sums, 0, keepdims=True)
    head = lax.broadcasted_iota(jnp.int32, (16, 128), 0)
    lane = lax.broadcasted_iota(jnp.int32, (16, 128), 1)
    pick = head == lane
    out = jnp.zeros((16, 128), jnp.float32)
    for d in range(16):
        col = jnp.sum(jnp.where(pick, jnp.broadcast_to(w[d], (16, 128)), 0.0), -1, keepdims=True)
        out = out + racc[d, b].astype(jnp.float32) * col
    o_ref[b] = out.astype(jnp.bfloat16)


def kernel(q_ref, k_hbm, v_hbm, o_ref, kbuf, vbuf, w_ref, s0, s1, p0, p1, st0, st1, racc, rst, ksem, vsem, asend, arecv, ssend, srecv):
    n = q_ref.shape[0]
    parts = racc.shape[0]
    bulk = n // GROUP - 1
    me = lax.axis_index("sp")
    s_refs, p_refs, st = (s0, s1), (p0, p1), (st0, st1)
    def kcopy(b):
        s = lax.rem(b, SLOTS)
        return pltpu.make_async_copy(k_hbm.at[b], kbuf.at[s], ksem.at[s])
    def vcopy(b):
        s = lax.rem(b, SLOTS)
        return pltpu.make_async_copy(v_hbm.at[b], vbuf.at[s], vsem.at[s])
    for b in range(SLOTS):
        kcopy(b).start(); vcopy(b).start()

    barrier = pltpu.get_barrier_semaphore()
    def peer(i):
        return {"sp": lax.rem(me + i, parts)}
    def greet(i, c):
        pl.semaphore_signal(barrier, inc=1, device_id=peer(i), device_id_type=MESH)
        return c
    lax.fori_loop(1, parts, greet, 0)
    w_ref[...] = jnp.zeros_like(w_ref)

    def copies(slot, start, size, g, i):
        seqs = pl.ds(start, size)
        return (
            pltpu.make_async_remote_copy(racc.at[slot, seqs], racc.at[slot, seqs], asend.at[g], arecv.at[g], device_id=peer(i), device_id_type=MESH),
            pltpu.make_async_remote_copy(rst.at[slot, seqs], rst.at[slot, seqs], ssend.at[g], srecv.at[g], device_id=peer(i), device_id_type=MESH),
        )
    def send(start, size, g):
        for i in range(1, parts):
            for c in copies(me, start, size, g, i):
                c.start()
    def arrived(start, size, g):
        for c in copies(pl.ds(0, parts - 1), start, size, g, 1):
            c.wait_recv()
    def sent(start, size, g):
        for c in copies(pl.ds(0, parts - 1), start, size, g, 1):
            c.wait_send()
    def fill(b):
        for j in range(8):
            w_ref[16*j:16*j+16, 128*j:128*j+128] = q_ref[b]
    def qk(b, h):
        s_refs[h][...] = scores(w_ref, kbuf[lax.rem(b, SLOTS), 256*h:256*h+256])
    def wt(h):
        p, high, total = weigh(s_refs[h][...], SCALE)
        p_refs[h][...] = p
        st[h][0] = jnp.broadcast_to(high, (16, 128))
        st[h][1] = jnp.broadcast_to(total, (16, 128))
    def pv(b, h):
        return mix(p_refs[h][...], vbuf[lax.rem(b, SLOTS), 256*h:256*h+256])
    def finish(b, o0, o1, h0, t0):
        h1, t1 = st[1][0], st[1][1]
        top = jnp.maximum(h0, h1)
        c0, c1 = jnp.exp2((h0 - top) * SCALE), jnp.exp2((h1 - top) * SCALE)
        racc[me, b] = (o0 * c0 + o1 * c1).astype(jnp.bfloat16)
        t = t0 * c0 + t1 * c1
        head = lax.broadcasted_iota(jnp.int32, (16, 128), 0)
        lane = lax.broadcasted_iota(jnp.int32, (16, 128), 1)
        rst[me, b] = jnp.sum(jnp.where(lane == head, top, jnp.where(lane == head + 16, t, 0.0)), 0, keepdims=True)

    def body(b, c):
        kcopy(b).wait()
        vcopy(b - 1).wait()
        fill(b)
        h0, t0 = st[0][0], st[0][1]
        o0 = pv(b - 1, 0)
        wt(1)
        qk(b, 0)
        o1 = pv(b - 1, 1)
        finish(b - 1, o0, o1, h0, t0)
        wt(0)
        qk(b, 1)
        @pl.when(b + SLOTS < n)
        def _():
            kcopy(b + SLOTS).start()
        @pl.when(b - 1 + SLOTS < n)
        def _():
            vcopy(b - 1 + SLOTS).start()
        @pl.when(b == GROUP)
        def _():
            pl.semaphore_wait(barrier, parts - 1)
        @pl.when((lax.rem(b, GROUP) == 0) & (b <= bulk * GROUP))
        def _():
            send(b - GROUP, GROUP, b // GROUP - 1)
        @pl.when((lax.rem(b, GROUP) == 0) & (b >= 2 * GROUP))
        def _():
            g = b // GROUP - 2
            arrived(g * GROUP, GROUP, g)
            for i in range(GROUP):
                combine(racc, rst, o_ref, g * GROUP + i)
        @pl.when(b == n - 2)
        def _():
            send(n - 4, 2, bulk)
        @pl.when(b == n - 1)
        def _():
            send(n - 2, 1, bulk + 1)
        return c
    kcopy(0).wait()
    fill(0)
    qk(0, 0)
    wt(0)
    qk(0, 1)
    kcopy(SLOTS).start()
    lax.fori_loop(1, n, body, 0)
    vcopy(n - 1).wait()
    h0, t0 = st[0][0], st[0][1]
    o0 = pv(n - 1, 0)
    wt(1)
    o1 = pv(n - 1, 1)
    finish(n - 1, o0, o1, h0, t0)
    send(n - 1, 1, bulk + 2)
    last = bulk - 1
    tail = [(last * GROUP, GROUP, last), (n - 4, 2, bulk), (n - 2, 1, bulk + 1), (n - 1, 1, bulk + 2)]
    for start, size, g in tail:
        arrived(start, size, g)
        for i in range(size):
            combine(racc, rst, o_ref, start + i)
    def drain(g, c):
        sent(g * GROUP, GROUP, g)
        return c
    lax.fori_loop(0, bulk, drain, 0)
    for start, size, g in tail[1:]:
        sent(start, size, g)

def solution(mesh):
    def step(q, k, v):
        n = q.shape[0]
        return pl.pallas_call(
            kernel,
            out_shape=jax.ShapeDtypeStruct(q.shape, jnp.bfloat16),
            in_specs=[pl.BlockSpec(memory_space=pltpu.VMEM), pl.BlockSpec(memory_space=pl.ANY), pl.BlockSpec(memory_space=pl.ANY)],
            out_specs=pl.BlockSpec(memory_space=pltpu.VMEM),
            scratch_shapes=[
                pltpu.VMEM((SLOTS, 512, 16, 128), jnp.bfloat16),
                pltpu.VMEM((SLOTS, 512, 16, 128), jnp.bfloat16),
                pltpu.VMEM((128, 1024), jnp.bfloat16),
                pltpu.VMEM((32, 16, 128), jnp.float32),
                pltpu.VMEM((32, 16, 128), jnp.float32),
                pltpu.VMEM((32, 16, 128), jnp.bfloat16),
                pltpu.VMEM((32, 16, 128), jnp.bfloat16),
                pltpu.VMEM((2, 16, 128), jnp.float32),
                pltpu.VMEM((2, 16, 128), jnp.float32),
                pltpu.VMEM((16, n, 16, 128), jnp.bfloat16),
                pltpu.VMEM((16, n, 1, 128), jnp.float32),
                pltpu.SemaphoreType.DMA((SLOTS,)),
                pltpu.SemaphoreType.DMA((SLOTS,)),
                pltpu.SemaphoreType.DMA((n // GROUP + 2,)),
                pltpu.SemaphoreType.DMA((n // GROUP + 2,)),
                pltpu.SemaphoreType.DMA((n // GROUP + 2,)),
                pltpu.SemaphoreType.DMA((n // GROUP + 2,)),
            ],
            compiler_params=pltpu.CompilerParams(vmem_limit_bytes=60 * 1024 * 1024, collective_id=0, has_side_effects=True),
        )(q, k, v)
    return jax.shard_map(step, mesh=mesh,
        in_specs=(P("dp", None, None), P("dp", "sp", None, None), P("dp", "sp", None, None)),
        out_specs=P("dp", None, None), check_vma=False)
```
